32 devices in a mesh: tile: 8 (over z, x), dir: 4 (over y, core).
Axes of the slice: x: 2, y: 2, z: 4, core: 2. Of those that a mesh axis runs over, the one named last changes fastest.
Arguments:
- probes: float32 [32, 64, 32, 128], P('dir', 'tile'), may hold values from -6 to 6
- base_sens: float32 [64, 32, 128], P('tile'), may hold values from -12 to 12
- obs_weight: float32 [64, 32, 128], P('tile'), may hold values from 1 to 10
- perm: float32 [64, 32, 128], P('tile'), may hold values from 0.25 to 4
- material: int32 [64, 32, 128], P('tile'), may hold values from 0 to 7
- class_storage: float32 [8], replicated, may hold values from 0.2 to 2
- class_alpha: float32 [8], replicated, may hold values from 0.5 to 1
- class_bulk: float32 [8], replicated, may hold values from 0.25 to 2
- class_shear: float32 [8], replicated, may hold values from 0.5 to 4
Outputs:
- hess_block: float32 [32, 64, 32, 128], P('dir', 'tile')
- r_factor: float32 [32, 32], replicated
The draws below stay inside these ranges and needn't reach their ends.
All inputs are finite; a program needn't handle non-finite values.
Results may differ from the reference program's by a relative error of at most 0.00016.
Values sent between devices are 32-bit elements; how exact they have to be, the bound alone decides.
A program may use at most 64 MiB of HBM per device.

```python
import math
import jax
import jax.numpy as jnp
from jax import lax

NY = 32
NZ = 128
DIR_DEV = 8
NCLASS = 8
SWEEPS = 2
STEPS = 2
NX = 64
DIRS = 32


def with_ends(drawn, key, low, largest):
    extent = drawn.shape
    index_at = [jax.random.randint(jax.random.fold_in(key, axis), (), 0, extent[axis]) for axis in range(len(extent))]
    drawn = drawn.at[tuple(index_at)].set(low)
    longest = extent.index(max(extent))
    index_at[longest] = (index_at[longest] + 1) % extent[longest]
    return drawn.at[tuple(index_at)].set(largest)


def shard_levels(own_key, shape, split, low, high):
    level = 1.0
    for dim, parts in split:
        steps = jax.random.uniform(jax.random.fold_in(jax.random.fold_in(own_key, 6), dim), (parts,), jnp.float32, low / len(split), high / len(split))
        level = level * jnp.repeat(jnp.exp(steps), shape[dim] // parts).reshape((-1,) + (1,) * (len(shape) - 1 - dim))
    return level


def scatter_about(rng, dims, scale, bound, split=(), kind=jnp.bfloat16):
    level = shard_levels(rng, dims, split, -0.22, 0.18) if split else 1.0
    drawn = jax.random.normal(rng, dims, jnp.float32) * scale * level
    return jnp.minimum(jnp.maximum(drawn, -bound), bound).astype(kind)


def setup_inputs(seed: int = 0) -> dict:
    seeds = jax.random.split(jax.random.key(seed), 10)
    probes = scatter_about(seeds[0], (DIRS, NX, NY, NZ), 1.0, 6.0, ((0, 4), (1, 8)), jnp.float32)
    base_sens = scatter_about(seeds[1], (NX, NY, NZ), 2.0, 12.0, ((0, 8),), jnp.float32)
    obs_weight = jnp.clip(jnp.exp(math.log(10.0) - 2.3025851 * jax.random.uniform(seeds[2], (NX, NY, NZ), jnp.float32) ** shard_levels(seeds[2], (NX, NY, NZ), ((0, 8),), -0.2, 0.2)), 1.0, 10.0)
    perm = jnp.clip(jnp.exp(math.log(4.0) - 2.7725887 * jax.random.uniform(seeds[3], (NX, NY, NZ), jnp.float32) ** shard_levels(seeds[3], (NX, NY, NZ), ((0, 8),), -0.2, 0.2)), 0.25, 4.0)
    material = with_ends(jax.random.randint(seeds[4], (NX, NY, NZ), 0, NCLASS), jax.random.fold_in(seeds[4], 1), 0, NCLASS - 1).astype(jnp.int32)
    class_storage = jnp.clip(jnp.exp(jax.random.uniform(seeds[5], (NCLASS,), jnp.float32, math.log(0.2), math.log(2.0))), 0.2, 2.0)
    class_alpha = jnp.clip(jax.random.uniform(seeds[6], (NCLASS,), jnp.float32, 0.5, 1.0), 0.5, 1.0)
    class_bulk = jnp.clip(jnp.exp(jax.random.uniform(seeds[7], (NCLASS,), jnp.float32, math.log(0.25), math.log(2.0))), 0.25, 2.0)
    class_shear = jnp.clip(jnp.exp(jax.random.uniform(seeds[8], (NCLASS,), jnp.float32, math.log(0.5), math.log(4.0))), 0.5, 4.0)
    return {"probes": probes, "base_sens": base_sens, "obs_weight": obs_weight, "perm": perm, "material": material, "class_storage": class_storage, "class_alpha": class_alpha, "class_bulk": class_bulk, "class_shear": class_shear}


def pad_first(field):
    return jnp.pad(field, [(0, 0)] * (field.ndim - 3) + [(1, 1), (0, 0), (0, 0)])

def pad_second(field):
    return jnp.pad(field, [(0, 0)] * (field.ndim - 2) + [(1, 1), (0, 0)])

def pad_third(field):
    return jnp.pad(field, [(0, 0)] * (field.ndim - 1) + [(1, 1)])

def face_flux(padded, coef_pad):
    center = padded[..., 1:-1, :, :]
    coef_mid = coef_pad[1:-1]
    result = 0.5 * (coef_mid + coef_pad[2:]) * (center - padded[..., 2:, :, :])
    result = result + 0.5 * (coef_mid + coef_pad[:-2]) * (center - padded[..., :-2, :, :])
    field_y = pad_second(center)
    coef_y = pad_second(coef_mid)
    result = result + 0.5 * (coef_mid + coef_y[:, 2:]) * (center - field_y[..., 2:, :])
    result = result + 0.5 * (coef_mid + coef_y[:, :-2]) * (center - field_y[..., :-2, :])
    field_z = pad_third(center)
    coef_z = pad_third(coef_mid)
    result = result + 0.5 * (coef_mid + coef_z[:, :, 2:]) * (center - field_z[..., 2:])
    result = result + 0.5 * (coef_mid + coef_z[:, :, :-2]) * (center - field_z[..., :-2])
    return result

def gradient(press_pad, biot):
    first = 0.5 * biot * (press_pad[..., 2:, :, :] - press_pad[..., :-2, :, :])
    center = press_pad[..., 1:-1, :, :]
    field_y = pad_second(center)
    second = 0.5 * biot * (field_y[..., 2:, :] - field_y[..., :-2, :])
    field_z = pad_third(center)
    third = 0.5 * biot * (field_z[..., 2:] - field_z[..., :-2])
    return jnp.stack([first, second, third])

def divergence(first_pad, others, biot_pad):
    weighted = biot_pad * first_pad
    result = 0.5 * (weighted[..., :-2, :, :] - weighted[..., 2:, :, :])
    biot = biot_pad[1:-1]
    second = pad_second(biot * others[0])
    result = result + 0.5 * (second[..., :-2, :] - second[..., 2:, :])
    third = pad_third(biot * others[1])
    result = result + 0.5 * (third[..., :-2] - third[..., 2:])
    return result

def inner(left, right):
    summed = lax.optimization_barrier(jnp.sum(left * right, axis=(-3, -2, -1)))
    if summed.ndim == 2:
        summed = lax.optimization_barrier(jnp.sum(summed, axis=0))
    return summed

def spread(values):
    return values[:, None, None, None]

def conj_grad(operate, target, iterate):
    if iterate is None:
        residual = target
        iterate = jnp.zeros_like(target)
    else:
        residual = target - operate(pad_first(iterate))
    direction = residual
    norm_now = inner(residual, residual)
    for step in range(STEPS):
        image = operate(pad_first(direction))
        step_len = norm_now / inner(direction, image)
        iterate = iterate + spread(step_len) * direction
        if step + 1 < STEPS:
            residual = residual - spread(step_len) * image
            norm_next = inner(residual, residual)
            direction = residual + spread(norm_next / norm_now) * direction
            norm_now = norm_next
    return iterate

def solve(source, orient, tables):
    perm_pad, biot, biot_pad, shear_pad, stab_term, diagonal = tables

    def press_apply(padded):
        return diagonal * padded[..., 1:-1, :, :] + face_flux(padded, perm_pad)

    def elast_apply(padded):
        return face_flux(padded, shear_pad)
    pressure = None
    displace = None
    for sweep in range(SWEEPS):
        source_term = source
        if displace is not None:
            source_term = source - orient * divergence(pad_first(displace[0]), (displace[1], displace[2]), biot_pad) + stab_term * pressure
        pressure = conj_grad(press_apply, source_term, pressure)
        elastic_term = orient * gradient(pad_first(pressure), biot)
        displace = conj_grad(elast_apply, elastic_term, displace)
    return pressure

def reference(probes, base_sens, obs_weight, perm, material, class_storage, class_alpha, class_bulk, class_shear):
    class_mask = (material[None] == jnp.arange(NCLASS, dtype=jnp.int32)[:, None, None, None]).astype(jnp.float32)
    storage = lax.optimization_barrier(jnp.sum(class_storage[:, None, None, None] * class_mask, axis=0))
    biot = lax.optimization_barrier(jnp.sum(class_alpha[:, None, None, None] * class_mask, axis=0))
    bulk = lax.optimization_barrier(jnp.sum(class_bulk[:, None, None, None] * class_mask, axis=0))
    shear = lax.optimization_barrier(jnp.sum(class_shear[:, None, None, None] * class_mask, axis=0))
    stab_term = biot * biot / bulk
    diagonal = storage + stab_term
    tables = (pad_first(perm), biot, pad_first(biot), pad_first(shear), stab_term, diagonal)

    def one_block(probe_block):
        tangent = solve(base_sens * probe_block, 1.0, tables)
        adjoint = solve(obs_weight * tangent, -1.0, tables)
        return base_sens * adjoint
    blocks = probes.reshape((-1, DIR_DEV) + probes.shape[1:])
    hess_block = lax.map(one_block, blocks).reshape(probes.shape)
    columns = hess_block.reshape(DIRS, -1)
    gram = jnp.dot(columns.astype(jnp.float32), columns.T.astype(jnp.float32), precision=lax.Precision.HIGHEST, preferred_element_type=jnp.float32) / (NX * NY * NZ)
    r_factor = jnp.linalg.cholesky(gram).T
    return (hess_block, r_factor)
```

```python
import functools

import jax
import jax.numpy as jnp
from jax import lax
from jax.experimental import pallas as pl
from jax.experimental.pallas import tpu as pltpu
from jax.sharding import PartitionSpec as P

NCLASS = 8
SWEEPS = 2
STEPS = 2


def extended(cells, sides, width):
    for axis, dim in sides:
        count = lax.axis_size(axis)
        ends = count - 1
        head = lax.slice_in_dim(cells, 0, width, axis=dim)
        tail = lax.slice_in_dim(cells, cells.shape[dim] - width, cells.shape[dim], axis=dim)
        cells = jnp.concatenate(
            [
                lax.ppermute(tail, axis, [(i, (i + 1) % count) for i in range(ends)]),
                cells,
                lax.ppermute(head, axis, [((i + 1) % count, i) for i in range(ends)]),
            ],
            axis=dim,
        )
    return cells


def pad_second(field):
    return jnp.pad(field, [(0, 0)] * (field.ndim - 2) + [(1, 1), (0, 0)])


def pad_third(field):
    return jnp.pad(field, [(0, 0)] * (field.ndim - 1) + [(1, 1)])


def face_flux(padded, coef_pad):
    center = padded[..., 1:-1, :, :]
    coef_mid = coef_pad[1:-1]
    result = 0.5 * (coef_mid + coef_pad[2:]) * (center - padded[..., 2:, :, :])
    result = result + 0.5 * (coef_mid + coef_pad[:-2]) * (center - padded[..., :-2, :, :])
    field_y = pad_second(center)
    coef_y = pad_second(coef_mid)
    result = result + 0.5 * (coef_mid + coef_y[:, 2:]) * (center - field_y[..., 2:, :])
    result = result + 0.5 * (coef_mid + coef_y[:, :-2]) * (center - field_y[..., :-2, :])
    field_z = pad_third(center)
    coef_z = pad_third(coef_mid)
    result = result + 0.5 * (coef_mid + coef_z[:, :, 2:]) * (center - field_z[..., 2:])
    result = result + 0.5 * (coef_mid + coef_z[:, :, :-2]) * (center - field_z[..., :-2])
    return result


def gradient(press_pad, biot):
    first = 0.5 * biot * (press_pad[..., 2:, :, :] - press_pad[..., :-2, :, :])
    center = press_pad[..., 1:-1, :, :]
    field_y = pad_second(center)
    second = 0.5 * biot * (field_y[..., 2:, :] - field_y[..., :-2, :])
    field_z = pad_third(center)
    third = 0.5 * biot * (field_z[..., 2:] - field_z[..., :-2])
    return jnp.stack([first, second, third])


def divergence(first_pad, others, biot_pad):
    weighted = biot_pad * first_pad
    result = 0.5 * (weighted[..., :-2, :, :] - weighted[..., 2:, :, :])
    biot = biot_pad[1:-1]
    second = pad_second(biot * others[0])
    result = result + 0.5 * (second[..., :-2, :] - second[..., 2:, :])
    third = pad_third(biot * others[1])
    result = result + 0.5 * (third[..., :-2] - third[..., 2:])
    return result


def inner(left, right):
    summed = jnp.sum(left * right, axis=(-3, -2, -1))
    if summed.ndim == 2:
        summed = jnp.sum(summed, axis=0)
    return lax.psum(summed, "tile")


def spread(values):
    return values[:, None, None, None]


def pad_scalar(field):
    return extended(field, (("tile", 1),), 1)


def pad_vector(field):
    return extended(field, (("tile", 2),), 1)


def conj_grad(operate, extend, target, iterate, iter_pad):
    if iterate is None:
        residual = target
        iterate = jnp.zeros_like(target)
    else:
        residual = target - operate(iter_pad)
    direction = residual
    norm_now = inner(residual, residual)
    for step in range(STEPS):
        image = operate(extend(direction))
        step_len = norm_now / inner(direction, image)
        iterate = iterate + spread(step_len) * direction
        if step + 1 < STEPS:
            residual = residual - spread(step_len) * image
            norm_next = inner(residual, residual)
            direction = residual + spread(norm_next / norm_now) * direction
            norm_now = norm_next
    return iterate


def halo_body(
    probes,
    base_sens,
    obs_weight,
    perm,
    material,
    class_storage,
    class_alpha,
    class_bulk,
    class_shear,
):
    class_mask = (
        material[None] == jnp.arange(NCLASS, dtype=jnp.int32)[:, None, None, None]
    ).astype(jnp.float32)
    storage = jnp.sum(class_storage[:, None, None, None] * class_mask, axis=0)
    biot = jnp.sum(class_alpha[:, None, None, None] * class_mask, axis=0)
    bulk = jnp.sum(class_bulk[:, None, None, None] * class_mask, axis=0)
    shear = jnp.sum(class_shear[:, None, None, None] * class_mask, axis=0)
    stab_term = biot * biot / bulk
    diagonal = storage + stab_term
    coef_all = extended(jnp.stack([perm, biot, shear]), (("tile", 1),), 1)
    perm_pad = coef_all[0]
    biot_pad = coef_all[1]
    shear_pad = coef_all[2]

    def press_apply(padded):
        return diagonal * padded[..., 1:-1, :, :] + face_flux(padded, perm_pad)

    def elast_apply(padded):
        return face_flux(padded, shear_pad)

    def solve(source, orient):
        pressure = None
        displace = None
        press_pad = None
        for sweep in range(SWEEPS):
            source_term = source
            press_init = None
            disp_pad = None
            if displace is not None:
                first_pad = pad_scalar(displace[0])
                press_init = pad_scalar(pressure)
                source_term = (
                    source
                    - orient * divergence(first_pad, (displace[1], displace[2]), biot_pad)
                    + stab_term * pressure
                )
            pressure = conj_grad(press_apply, pad_scalar, source_term, pressure, press_init)
            press_pad = pad_scalar(pressure)
            elastic_term = orient * gradient(press_pad, biot)
            if displace is not None and disp_pad is None:
                disp_pad = pad_vector(displace)
            displace = conj_grad(elast_apply, pad_vector, elastic_term, displace, disp_pad)
        return pressure

    tangent = solve(base_sens * probes, 1.0)
    adjoint = solve(obs_weight * tangent, -1.0)
    hess_block = base_sens * adjoint
    cell_count = (
        hess_block.shape[1] * lax.axis_size("tile") * hess_block.shape[2] * hess_block.shape[3]
    )
    regrouped = lax.all_to_all(hess_block, "dir", split_axis=2, concat_axis=0, tiled=True)
    columns = regrouped.reshape(regrouped.shape[0], -1)
    gram_local = (
        jnp.dot(
            columns, columns.T, precision=lax.Precision.HIGHEST, preferred_element_type=jnp.float32
        )
        / cell_count
    )
    gram_whole = lax.psum(gram_local, ("tile", "dir"))
    r_factor = jnp.linalg.cholesky(gram_whole).T
    return (hess_block, r_factor)

MESH = pl.DeviceIdType.MESH
SUBL = 8
LANES = 128
PAD = 8


def whole_sum(acc):
    return jnp.sum(jnp.sum(acc, axis=1, keepdims=True), axis=0, keepdims=True)


def kernel(
    dims,
    tables,
    src_in,
    pm_in,
    obs_in,
    bs_in,
    adj,
    r_out,
    src_all,
    pm_all,
    obs_all,
    out_all,
    gat,
    ycol,
    part_dir,
    part_tile,
    perm_f,
    shear_f,
    diag_f,
    stab_f,
    hb_f,
    pcs,
    pcx,
    pcy,
    pcz,
    ecs,
    ecx,
    ecy,
    ecz,
    r0,
    r1,
    pb,
    wb,
    tb,
    eb,
    fb,
    we,
    pm_send,
    pm_recv,
    fw_send,
    fw_recv,
    src_send,
    src_recv,
    obs_send,
    obs_recv,
    ret_send,
    ret_recv,
    y_send,
    y_recv,
    g_send,
    g_recv,
    t_send,
    t_recv,
    own_sem,
):
    nt, nd, nx, ny, cells = dims
    rows = nx * ny
    half = rows // 2
    quarter = rows // nd
    pitch = rows + PAD
    pm_pitch = 2 * rows + PAD
    gpitch = quarter + PAD
    me = lax.axis_index("tile")
    q = lax.axis_index("dir")
    core = lax.rem(q, 2)
    partner = q + 1 - 2 * core

    def span(start, size):
        return pl.ds(pl.multiple_of(start, 8), size)

    def ahead(k):
        return lax.rem(me + k, nt)

    def behind(k):
        return lax.rem(me + nt - k, nt)

    barrier = pltpu.get_barrier_semaphore()
    for k in range(1, nt):
        pl.semaphore_signal(barrier, inc=1, device_id={"tile": ahead(k)}, device_id_type=MESH)
    for m in range(1, nd):
        pl.semaphore_signal(
            barrier, inc=1, device_id={"dir": lax.rem(q + m, nd)}, device_id_type=MESH
        )
    pl.semaphore_wait(barrier, nt + nd - 2)

    def remote(src, dst, send, recv, axis, to):
        return pltpu.make_async_remote_copy(
            src_ref=src,
            dst_ref=dst,
            send_sem=send,
            recv_sem=recv,
            device_id={axis: to},
            device_id_type=MESH,
        )

    def pm_copy(k, owner, to):
        return remote(
            pm_in.at[span(core * rows, rows)],
            pm_all.at[span(owner * pm_pitch + core * rows, rows)],
            pm_send.at[k],
            pm_recv.at[k],
            "tile",
            to,
        )

    def src_copy(k, owner, to):
        return remote(
            src_in.at[span(to * rows, rows)],
            src_all.at[span(owner * pitch, rows)],
            src_send.at[k],
            src_recv.at[k],
            "tile",
            to,
        )

    def obs_copy(k, owner, to):
        return remote(
            obs_in, obs_all.at[span(owner * pitch, rows)], obs_send.at[k], obs_recv.at[k], "tile", to
        )

    def fw_copy(k, which):
        owner = behind(k)
        place = pm_all.at[span(owner * pm_pitch + which * rows, rows)]
        source = pm_in.at[span(which * rows, rows)] if k == 0 else place
        return remote(source, place, fw_send.at[k], fw_recv.at[k], "dir", partner)

    for k in range(1, nt):
        pm_copy(k, me, ahead(k)).start()
    for k in range(1, nt):
        src_copy(k, me, ahead(k)).start()
    own = [
        pltpu.make_async_copy(
            pm_in.at[span(core * rows, rows)],
            pm_all.at[span(me * pm_pitch + core * rows, rows)],
            own_sem.at[0],
        ),
        pltpu.make_async_copy(
            src_in.at[span(me * rows, rows)], src_all.at[span(me * pitch, rows)], own_sem.at[1]
        ),
        pltpu.make_async_copy(obs_in, obs_all.at[span(me * pitch, rows)], own_sem.at[2]),
    ]
    for copy in own:
        copy.start()
    fw_copy(0, core).start()
    for k in range(1, nt):
        pm_copy(k, behind(k), behind(k)).wait_recv()
        fw_copy(k, core).start()
    own[0].wait()
    for k in range(nt):
        fw_copy(k, 1 - core).wait_recv()

    sub = lax.broadcasted_iota(jnp.int32, (SUBL, LANES), 0)
    lane = lax.broadcasted_iota(jnp.int32, (SUBL, LANES), 1)
    sub_lo, sub_hi = sub > 0, sub < SUBL - 1
    lane_lo, lane_hi = lane > 0, lane < LANES - 1
    zero = jnp.zeros((SUBL, LANES), jnp.float32)

    def down(v):
        return jnp.where(sub_lo, pltpu.roll(v, 1, 0), 0.0)

    def up(v):
        return jnp.where(sub_hi, pltpu.roll(v, SUBL - 1, 0), 0.0)

    def next_z(v):
        return pltpu.roll(v, LANES - 1, 1)

    def prev_z(v):
        return pltpu.roll(v, 1, 1)

    def halo(field):
        for y in range(ny):
            field[0, y] = down(field[nx, y])
            field[nx + 1, y] = up(field[1, y])

    def planes(step, init):
        return lax.fori_loop(0, nx, step, init)

    half_planes = nx // 2

    def lookup(x, _):
        block = x // half_planes
        inside = x - block * half_planes
        base = block * rows + inside * ny
        for y in range(ny):
            perm_f[x + 1, y] = pm_all[pl.ds(base + y, SUBL, stride=pm_pitch), :]
            mat = pm_all[pl.ds(base + half + y, SUBL, stride=pm_pitch), :]
            storage, alpha, bulk, shear = zero, zero, zero, zero
            for c in range(NCLASS):
                hit = mat == float(c)
                storage = jnp.where(hit, tables[0, c], storage)
                alpha = jnp.where(hit, tables[1, c], alpha)
                bulk = jnp.where(hit, tables[2, c], bulk)
                shear = jnp.where(hit, tables[3, c], shear)
            stab = alpha * alpha / bulk
            stab_f[x, y] = stab
            diag_f[x, y] = storage + stab
            hb_f[x, y] = 0.5 * alpha
            shear_f[x + 1, y] = shear
        return 0

    planes(lookup, 0)

    for coef, cs, cx, cy, cz, diag in (
        (perm_f, pcs, pcx, pcy, pcz, diag_f),
        (shear_f, ecs, ecx, ecy, ecz, None),
    ):
        halo(coef)

        def faces(x, _):
            for y in range(ny):
                mid = coef[x + 1, y]
                after = coef[x + 2, y]
                total = coef[x, y] + after
                nz_val = jnp.where(lane_hi, next_z(mid), 0.0)
                total = total + nz_val + jnp.where(lane_lo, prev_z(mid), 0.0)
                if y > 0:
                    total = total + coef[x + 1, y - 1]
                if y < ny - 1:
                    right = coef[x + 1, y + 1]
                    total = total + right
                    cy[x, y] = 0.5 * (mid + right)
                else:
                    cy[x, y] = zero
                cz[x, y] = jnp.where(lane_hi, 0.5 * (mid + nz_val), 0.0)
                face = 0.5 * (mid + after)
                cx[x + 1, y] = jnp.where(jnp.logical_or(x < nx - 1, sub_hi), face, 0.0)
                value = 3.0 * mid + 0.5 * total
                if diag is not None:
                    value = value + diag[x, y]
                cs[x, y] = value
            return 0

        planes(faces, 0)
        for y in range(ny):
            cx[0, y] = down(cx[nx, y])

    def stencil(fields, index, coefs, x, emit, carry):
        cs, cx, cy, cz = coefs
        count = len(index)
        before = [None] * count
        here = [fields(i, x + 1, 0) for i in range(count)]
        cy_before = None
        for y in range(ny):
            s, c_next, c_prev = cs[x, y], cx[x + 1, y], cx[x, y]
            c_y, c_z = cy[x, y], cz[x, y]
            images = []
            centers = []
            for i in range(count):
                v = here[i]
                out = s * v - c_next * fields(i, x + 2, y) - c_prev * fields(i, x, y)
                out = out - (c_z * next_z(v) + prev_z(c_z * v))
                if y > 0:
                    out = out - cy_before * before[i]
                after = None
                if y < ny - 1:
                    after = fields(i, x + 1, y + 1)
                    out = out - c_y * after
                images.append(out)
                centers.append(v)
                before[i], here[i] = v, after
            cy_before = c_y
            carry = emit(y, centers, images, carry)
        return carry

    def single(field):
        return lambda i, x, y: field[x, y]

    def triple(field):
        return lambda i, x, y: field[i, x, y]

    press = (pcs, pcx, pcy, pcz)
    elast = (ecs, ecx, ecy, ecz)

    def first_apply(fields, index, coefs, store):
        def step(x, carry):
            def emit(y, centers, images, acc):
                a, b = acc
                for i in index:
                    store(i, x, y, images[i])
                    a = a + centers[i] * centers[i]
                    b = b + centers[i] * images[i]
                return a, b

            return stencil(fields, index, coefs, x, emit, carry)

        a, b = planes(step, (zero, zero))
        return whole_sum(a), whole_sum(b)

    def second_apply(fields, olds, oldw, index, coefs, beta, store):
        def step(x, carry):
            def emit(y, centers, images, acc):
                for i in index:
                    w = images[i] + beta * oldw(i, x, y)
                    d = centers[i] + beta * olds(i, x + 1, y)
                    acc = acc + d * w
                    if store is not None:
                        store(i, x, y, w)
                return acc

            return stencil(fields, index, coefs, x, emit, carry)

        return whole_sum(planes(step, zero))

    def wb_store(i, x, y, value):
        wb[x, y] = value

    def we_store(i, x, y, value):
        we[i, x, y] = value

    def press_steps(keep):
        halo(r0)
        rr, rw = first_apply(single(r0), (0,), press, wb_store)
        a0 = rr / rw

        def residual(x, acc):
            for y in range(ny):
                v = r0[x + 1, y] - a0 * wb[x, y]
                r1[x + 1, y] = v
                acc = acc + v * v
            return acc

        rr1 = whole_sum(planes(residual, zero))
        beta = rr1 / rr
        halo(r1)
        dw = second_apply(
            single(r1),
            single(r0),
            lambda i, x, y: wb[x, y],
            (0,),
            press,
            beta,
            wb_store if keep else None,
        )
        return a0, rr1 / dw, beta

    for k in range(1, nt):
        src_copy(k, behind(k), behind(k)).wait_recv()
    own[1].wait()
    for k in range(1, nt):
        obs_copy(k, me, ahead(k)).start()

    def take_source(x, _):
        for y in range(ny):
            r0[x + 1, y] = src_all[pl.ds(x * ny + y, SUBL, stride=pitch), :]
        return 0

    planes(take_source, 0)

    def solve(turn, _):
        a0, a1, beta = press_steps(True)
        c0 = a0 + a1 * beta

        def first_press(x, _):
            for y in range(ny):
                old = r1[x + 1, y]
                p = c0 * r0[x + 1, y] + a1 * old
                pb[x + 1, y] = p
                tb[x, y] = old - a1 * wb[x, y] + stab_f[x, y] * p
            return 0

        planes(first_press, 0)
        halo(pb)

        def grad(x, _):
            for y in range(ny):
                b = hb_f[x, y]
                v = pb[x + 1, y]
                eb[0, x + 1, y] = b * (pb[x + 2, y] - pb[x, y])
                hi = pb[x + 1, y + 1] if y < ny - 1 else zero
                lo = pb[x + 1, y - 1] if y > 0 else zero
                eb[1, x + 1, y] = b * (hi - lo)
                eb[2, x + 1, y] = b * (
                    jnp.where(lane_hi, next_z(v), 0.0) - jnp.where(lane_lo, prev_z(v), 0.0)
                )
            return 0

        planes(grad, 0)
        for i in range(3):
            halo(eb.at[i])
        comps = (0, 1, 2)
        rr, rw = first_apply(triple(eb), comps, elast, we_store)
        b0 = rr / rw

        def residual(x, acc):
            for y in range(ny):
                for i in comps:
                    v = eb[i, x + 1, y] - b0 * we[i, x, y]
                    fb[i, x + 1, y] = v
                    acc = acc + v * v
            return acc

        rr1 = whole_sum(planes(residual, zero))
        beta_e = rr1 / rr
        for i in range(3):
            halo(fb.at[i])
        dw = second_apply(
            triple(fb), triple(eb), lambda i, x, y: we[i, x, y], comps, elast, beta_e, None
        )
        b1 = rr1 / dw
        e0 = b0 + b1 * beta_e

        def weigh(x, _):
            for y in range(ny):
                b = hb_f[x, y]
                for i in comps:
                    eb[i, x + 1, y] = b * (e0 * eb[i, x + 1, y] + b1 * fb[i, x + 1, y])
            return 0

        planes(weigh, 0)
        halo(eb.at[0])

        def next_source(x, _):
            for y in range(ny):
                total = tb[x, y] - (eb[0, x, y] - eb[0, x + 2, y])
                if y > 0:
                    total = total - eb[1, x + 1, y - 1]
                if y < ny - 1:
                    total = total + eb[1, x + 1, y + 1]
                w = eb[2, x + 1, y]
                total = total - (
                    jnp.where(lane_lo, prev_z(w), 0.0) - jnp.where(lane_hi, next_z(w), 0.0)
                )
                r0[x + 1, y] = total
            return 0

        planes(next_source, 0)
        a0, a1, beta = press_steps(False)
        c0 = a0 + a1 * beta

        @pl.when(turn == 0)
        def _():
            for k in range(1, nt):
                obs_copy(k, behind(k), behind(k)).wait_recv()
            own[2].wait()

            def last_press(x, _):
                for y in range(ny):
                    p = pb[x + 1, y] + c0 * r0[x + 1, y] + a1 * r1[x + 1, y]
                    r0[x + 1, y] = p * obs_all[pl.ds(x * ny + y, SUBL, stride=pitch), :]
                return 0

            planes(last_press, 0)

        @pl.when(turn == 1)
        def _():
            def last_press(x, _):
                for y in range(ny):
                    p = pb[x + 1, y] + c0 * r0[x + 1, y] + a1 * r1[x + 1, y]
                    out_all[pl.ds(x * ny + y, SUBL, stride=pitch), :] = p
                return 0

            planes(last_press, 0)

        return 0

    lax.fori_loop(0, 2, solve, 0)

    order = [nd // 2] + [m for m in range(1, nd) if m != nd // 2] + [0]

    def ret_copy(m, k, owner, to):
        chunk = lax.rem(q + m, nd)
        return remote(
            out_all.at[span(to * pitch + chunk * quarter, quarter)],
            adj.at[span(owner * rows + chunk * quarter, quarter)],
            ret_send.at[m, k],
            ret_recv.at[m, k],
            "tile",
            to,
        )

    def own_copy(m):
        chunk = lax.rem(q + m, nd)
        return pltpu.make_async_copy(
            out_all.at[span(me * pitch + chunk * quarter, quarter)],
            adj.at[span(me * rows + chunk * quarter, quarter)],
            own_sem.at[m],
        )

    def y_copy(m, k, group, chunk, to):
        owner = behind(k)
        return remote(
            adj.at[span(owner * rows + chunk * quarter, quarter)],
            gat.at[span((group * nt + owner) * gpitch, quarter)],
            y_send.at[m, k],
            y_recv.at[m, k],
            "dir",
            to,
        )

    for m in order:
        own_copy(m).start()
        for k in range(1, nt):
            ret_copy(m, k, me, ahead(k)).start()
    for m in order:
        to = lax.rem(q + m, nd)
        for k in range(nt):
            if k == 0:
                own_copy(m).wait()
            else:
                ret_copy(m, k, behind(k), behind(k)).wait_recv()
            if m > 0:
                y_copy(m, k, q, to, to).start()

    def columns(source, stride, base, group):
        def fill(r, _):
            value = source[pl.ds(base + r, SUBL, stride=stride), :]
            scale = bs_in[pl.ds(q * quarter + r, 1), :]
            ycol[span(group * SUBL, SUBL), pl.ds(pl.multiple_of(r * LANES, LANES), LANES)] = (
                value * scale
            )
            return 0

        lax.fori_loop(0, quarter, fill, 0, unroll=8)

    columns(adj, rows, q * quarter, q)
    for m in order[:-1]:
        group = lax.rem(q + nd - m, nd)
        for k in range(nt):
            y_copy(m, k, group, q, group).wait_recv()
        columns(gat, gpitch, group * nt * gpitch, group)

    nall = nd * nt
    gram = lax.dot_general(
        ycol[...],
        ycol[...],
        (((1,), (1,)), ((), ())),
        precision=lax.Precision.HIGHEST,
        preferred_element_type=jnp.float32,
    )

    def gather_sum(slots, place, send, recv, axis, count):
        def copy(k, owner, to):
            return remote(slots.at[owner], slots.at[owner], send.at[k], recv.at[k], axis, to)

        for k in range(1, count):
            copy(k, place, lax.rem(place + k, count)).start()
        for k in range(1, count):
            owner = lax.rem(place + count - k, count)
            copy(k, owner, owner).wait_recv()
        total = slots[0]
        for s in range(1, count):
            total = total + slots[s]
        for k in range(1, count):
            copy(k, place, lax.rem(place + k, count)).wait_send()
        return total

    part_dir[q] = jnp.zeros((nall, LANES), jnp.float32)
    part_dir[q, :, 0:nall] = gram
    part_tile[me] = gather_sum(part_dir, q, g_send, g_recv, "dir", nd)
    mat = gather_sum(part_tile, me, t_send, t_recv, "tile", nt) / cells

    lanes_all = lax.broadcasted_iota(jnp.int32, (1, LANES), 1)
    for j in range(nall):
        root = jnp.sqrt(mat[j : j + 1, j : j + 1])
        row = mat[j : j + 1, :] / root
        r_out[j : j + 1, :] = jnp.where(lanes_all >= j, row, 0.0)[:, 0:nall]
        mat = mat - (mat[:, j : j + 1] / root) * row

    for k in range(1, nt):
        pm_copy(k, me, ahead(k)).wait_send()
        src_copy(k, me, ahead(k)).wait_send()
        obs_copy(k, me, ahead(k)).wait_send()
        for m in order:
            ret_copy(m, k, me, ahead(k)).wait_send()
    for k in range(nt):
        fw_copy(k, core).wait_send()
        for m in order[:-1]:
            to = lax.rem(q + m, nd)
            y_copy(m, k, q, to, to).wait_send()


def local_body(
    probes,
    base_sens,
    obs_weight,
    perm,
    material,
    class_storage,
    class_alpha,
    class_bulk,
    class_shear,
):
    nt, nd = lax.axis_size("tile"), lax.axis_size("dir")
    count, nx, ny, nz = probes.shape
    rows = nx * ny
    tables = jnp.stack([class_storage, class_alpha, class_bulk, class_shear])
    source = (base_sens * probes).reshape(count * rows, nz)
    coefs = jnp.stack(
        [
            perm.reshape(2, rows // 2, nz),
            material.astype(jnp.float32).reshape(2, rows // 2, nz),
        ],
        axis=1,
    ).reshape(2 * rows, nz)
    nall = nd * count
    quarter = rows // nd
    vmem = pl.BlockSpec(memory_space=pltpu.VMEM)
    f32 = jnp.float32

    def rowbuf(n):
        return pltpu.VMEM((n, nz), f32)

    def field(n):
        return pltpu.VMEM((n, ny, SUBL, LANES), f32)

    def fields(n):
        return pltpu.VMEM((3, n, ny, SUBL, LANES), f32)

    sems = pltpu.SemaphoreType.DMA
    inner_f, outer_f = field(nx), field(nx + 2)
    scratch = [
        rowbuf(nt * (rows + PAD)),
        rowbuf(nt * (2 * rows + PAD)),
        rowbuf(nt * (rows + PAD)),
        rowbuf(nt * (rows + PAD)),
        rowbuf(nall * (quarter + PAD)),
        pltpu.VMEM((nall, quarter * nz), f32),
        pltpu.VMEM((nd, nall, LANES), f32),
        pltpu.VMEM((nt, nall, LANES), f32),
        outer_f,
        outer_f,
        inner_f,
        inner_f,
        inner_f,
        inner_f,
        field(nx + 1),
        inner_f,
        inner_f,
        inner_f,
        field(nx + 1),
        inner_f,
        inner_f,
        outer_f,
        outer_f,
        outer_f,
        inner_f,
        inner_f,
        fields(nx + 2),
        fields(nx + 2),
        fields(nx),
        sems((nt,)),
        sems((nt,)),
        sems((nt,)),
        sems((nt,)),
        sems((nt,)),
        sems((nt,)),
        sems((nt,)),
        sems((nt,)),
        sems((nd, nt)),
        sems((nd, nt)),
        sems((nd, nt)),
        sems((nd, nt)),
        sems((nd,)),
        sems((nd,)),
        sems((nt,)),
        sems((nt,)),
        sems((max(nd, 3),)),
    ]
    adjoint, r_factor = pl.pallas_call(
        functools.partial(kernel, (nt, nd, nx, ny, float(nt * rows * nz))),
        out_shape=(
            jax.ShapeDtypeStruct((count * rows, nz), f32),
            jax.ShapeDtypeStruct((nall, nall), f32),
        ),
        in_specs=[pl.BlockSpec(memory_space=pltpu.SMEM)] + [vmem] * 4,
        out_specs=(vmem, vmem),
        scratch_shapes=scratch,
        compiler_params=pltpu.CompilerParams(
            collective_id=0, has_side_effects=True, vmem_limit_bytes=60 * 1024 * 1024
        ),
    )(tables, source, coefs, obs_weight.reshape(rows, nz), base_sens.reshape(rows, nz))
    return (base_sens * adjoint.reshape(probes.shape), r_factor)


def body(probes, *others):
    nt, nd = lax.axis_size("tile"), lax.axis_size("dir")
    count, nx, ny, nz = probes.shape
    fits = nt == SUBL and count == nt and nz == LANES and nd % 2 == 0 and nx % 2 == 0
    fits = fits and ny % 8 == 0 and (nx * ny) % (8 * nd) == 0 and nd * nt <= LANES
    fits = fits and nx * ny * nz <= 32768
    return (local_body if fits else halo_body)(probes, *others)


def solution(mesh):
    placed = (
        P("dir", "tile", None, None),
        P("tile", None, None),
        P("tile", None, None),
        P("tile", None, None),
        P("tile", None, None),
        P(),
        P(),
        P(),
        P(),
    )
    return jax.shard_map(
        body,
        mesh=mesh,
        in_specs=placed,
        out_specs=(P("dir", "tile", None, None), P()),
        check_vma=False,
    )
```

```python
import functools

import jax
import jax.numpy as jnp
from jax import lax
from jax.experimental import pallas as pl
from jax.experimental.pallas import tpu as pltpu
from jax.sharding import PartitionSpec as P

NCLASS = 8
SWEEPS = 2
STEPS = 2


def extended(cells, sides, width):
    for axis, dim in sides:
        count = lax.axis_size(axis)
        ends = count - 1
        head = lax.slice_in_dim(cells, 0, width, axis=dim)
        tail = lax.slice_in_dim(cells, cells.shape[dim] - width, cells.shape[dim], axis=dim)
        cells = jnp.concatenate(
            [
                lax.ppermute(tail, axis, [(i, (i + 1) % count) for i in range(ends)]),
                cells,
                lax.ppermute(head, axis, [((i + 1) % count, i) for i in range(ends)]),
            ],
            axis=dim,
        )
    return cells


def pad_second(field):
    return jnp.pad(field, [(0, 0)] * (field.ndim - 2) + [(1, 1), (0, 0)])


def pad_third(field):
    return jnp.pad(field, [(0, 0)] * (field.ndim - 1) + [(1, 1)])


def face_flux(padded, coef_pad):
    center = padded[..., 1:-1, :, :]
    coef_mid = coef_pad[1:-1]
    result = 0.5 * (coef_mid + coef_pad[2:]) * (center - padded[..., 2:, :, :])
    result = result + 0.5 * (coef_mid + coef_pad[:-2]) * (center - padded[..., :-2, :, :])
    field_y = pad_second(center)
    coef_y = pad_second(coef_mid)
    result = result + 0.5 * (coef_mid + coef_y[:, 2:]) * (center - field_y[..., 2:, :])
    result = result + 0.5 * (coef_mid + coef_y[:, :-2]) * (center - field_y[..., :-2, :])
    field_z = pad_third(center)
    coef_z = pad_third(coef_mid)
    result = result + 0.5 * (coef_mid + coef_z[:, :, 2:]) * (center - field_z[..., 2:])
    result = result + 0.5 * (coef_mid + coef_z[:, :, :-2]) * (center - field_z[..., :-2])
    return result


def gradient(press_pad, biot):
    first = 0.5 * biot * (press_pad[..., 2:, :, :] - press_pad[..., :-2, :, :])
    center = press_pad[..., 1:-1, :, :]
    field_y = pad_second(center)
    second = 0.5 * biot * (field_y[..., 2:, :] - field_y[..., :-2, :])
    field_z = pad_third(center)
    third = 0.5 * biot * (field_z[..., 2:] - field_z[..., :-2])
    return jnp.stack([first, second, third])


def divergence(first_pad, others, biot_pad):
    weighted = biot_pad * first_pad
    result = 0.5 * (weighted[..., :-2, :, :] - weighted[..., 2:, :, :])
    biot = biot_pad[1:-1]
    second = pad_second(biot * others[0])
    result = result + 0.5 * (second[..., :-2, :] - second[..., 2:, :])
    third = pad_third(biot * others[1])
    result = result + 0.5 * (third[..., :-2] - third[..., 2:])
    return result


def inner(left, right):
    summed = jnp.sum(left * right, axis=(-3, -2, -1))
    if summed.ndim == 2:
        summed = jnp.sum(summed, axis=0)
    return lax.psum(summed, "tile")


def spread(values):
    return values[:, None, None, None]


def pad_scalar(field):
    return extended(field, (("tile", 1),), 1)


def pad_vector(field):
    return extended(field, (("tile", 2),), 1)


def conj_grad(operate, extend, target, iterate, iter_pad):
    if iterate is None:
        residual = target
        iterate = jnp.zeros_like(target)
    else:
        residual = target - operate(iter_pad)
    direction = residual
    norm_now = inner(residual, residual)
    for step in range(STEPS):
        image = operate(extend(direction))
        step_len = norm_now / inner(direction, image)
        iterate = iterate + spread(step_len) * direction
        if step + 1 < STEPS:
            residual = residual - spread(step_len) * image
            norm_next = inner(residual, residual)
            direction = residual + spread(norm_next / norm_now) * direction
            norm_now = norm_next
    return iterate


def halo_body(
    probes,
    base_sens,
    obs_weight,
    perm,
    material,
    class_storage,
    class_alpha,
    class_bulk,
    class_shear,
):
    class_mask = (
        material[None] == jnp.arange(NCLASS, dtype=jnp.int32)[:, None, None, None]
    ).astype(jnp.float32)
    storage = jnp.sum(class_storage[:, None, None, None] * class_mask, axis=0)
    biot = jnp.sum(class_alpha[:, None, None, None] * class_mask, axis=0)
    bulk = jnp.sum(class_bulk[:, None, None, None] * class_mask, axis=0)
    shear = jnp.sum(class_shear[:, None, None, None] * class_mask, axis=0)
    stab_term = biot * biot / bulk
    diagonal = storage + stab_term
    coef_all = extended(jnp.stack([perm, biot, shear]), (("tile", 1),), 1)
    perm_pad = coef_all[0]
    biot_pad = coef_all[1]
    shear_pad = coef_all[2]

    def press_apply(padded):
        return diagonal * padded[..., 1:-1, :, :] + face_flux(padded, perm_pad)

    def elast_apply(padded):
        return face_flux(padded, shear_pad)

    def solve(source, orient):
        pressure = None
        displace = None
        press_pad = None
        for sweep in range(SWEEPS):
            source_term = source
            press_init = None
            disp_pad = None
            if displace is not None:
                first_pad = pad_scalar(displace[0])
                press_init = pad_scalar(pressure)
                source_term = (
                    source
                    - orient * divergence(first_pad, (displace[1], displace[2]), biot_pad)
                    + stab_term * pressure
                )
            pressure = conj_grad(press_apply, pad_scalar, source_term, pressure, press_init)
            press_pad = pad_scalar(pressure)
            elastic_term = orient * gradient(press_pad, biot)
            if displace is not None and disp_pad is None:
                disp_pad = pad_vector(displace)
            displace = conj_grad(elast_apply, pad_vector, elastic_term, displace, disp_pad)
        return pressure

    tangent = solve(base_sens * probes, 1.0)
    adjoint = solve(obs_weight * tangent, -1.0)
    hess_block = base_sens * adjoint
    cell_count = (
        hess_block.shape[1] * lax.axis_size("tile") * hess_block.shape[2] * hess_block.shape[3]
    )
    regrouped = lax.all_to_all(hess_block, "dir", split_axis=2, concat_axis=0, tiled=True)
    columns = regrouped.reshape(regrouped.shape[0], -1)
    gram_local = (
        jnp.dot(
            columns, columns.T, precision=lax.Precision.HIGHEST, preferred_element_type=jnp.float32
        )
        / cell_count
    )
    gram_whole = lax.psum(gram_local, ("tile", "dir"))
    r_factor = jnp.linalg.cholesky(gram_whole).T
    return (hess_block, r_factor)

MESH = pl.DeviceIdType.MESH
SUBL = 8
LANES = 128
PAD = 8


def whole_sum(acc):
    return jnp.sum(jnp.sum(acc, axis=1, keepdims=True), axis=0, keepdims=True)


def kernel(
    dims,
    tables,
    src_in,
    pm_in,
    bs_in,
    adj,
    r_out,
    src_all,
    pm_all,
    out_all,
    gat,
    ycol,
    part_dir,
    part_tile,
    perm_f,
    shear_f,
    diag_f,
    stab_f,
    hb_f,
    pcs,
    pcx,
    pcy,
    pcz,
    ecs,
    ecx,
    ecy,
    ecz,
    r0,
    r1,
    pb,
    wb,
    tb,
    eb,
    fb,
    we,
    col_send,
    col_recv,
    row_send,
    row_recv,
    dir_send,
    dir_recv,
    core_send,
    core_recv,
    src_send,
    src_recv,
    ret_send,
    ret_recv,
    y_send,
    y_recv,
    g_send,
    g_recv,
    t_send,
    t_recv,
    own_sem,
):
    nt, nd, nx, ny, cells = dims
    rows = nx * ny
    quarter = rows // nd
    piece = 3 * quarter
    pitch = rows + PAD
    pm_pitch = 3 * rows + PAD
    gpitch = quarter + PAD
    me = lax.axis_index("tile")
    q = lax.axis_index("dir")
    core = lax.rem(q, 2)
    partner = q + 1 - 2 * core
    across = lax.rem(q + nd // 2, nd)
    mate = me + 1 - 2 * lax.rem(me, 2)

    def span(start, size):
        return pl.ds(pl.multiple_of(start, 8), size)

    def ahead(k):
        return lax.rem(me + k, nt)

    def behind(k):
        return lax.rem(me + nt - k, nt)

    barrier = pltpu.get_barrier_semaphore()
    for k in range(1, nt):
        pl.semaphore_signal(barrier, inc=1, device_id={"tile": ahead(k)}, device_id_type=MESH)
    for m in range(1, nd):
        pl.semaphore_signal(
            barrier, inc=1, device_id={"dir": lax.rem(q + m, nd)}, device_id_type=MESH
        )
    pl.semaphore_wait(barrier, nt + nd - 2)

    def remote(src, dst, send, recv, axis, to):
        return pltpu.make_async_remote_copy(
            src_ref=src,
            dst_ref=dst,
            send_sem=send,
            recv_sem=recv,
            device_id={axis: to},
            device_id_type=MESH,
        )

    def place(owner, part):
        return pm_all.at[span(owner * pm_pitch + part * piece, piece)]

    mine = pm_in.at[span(q * piece, piece)]

    def col_copy(k, owner, to):
        return remote(mine, place(owner, q), col_send.at[k], col_recv.at[k], "tile", to)

    def row_copy(k, base, to):
        owner = lax.rem(base + nt - k, nt)
        return remote(
            mine if k == 0 else place(owner, q),
            place(owner, q),
            row_send.at[k],
            row_recv.at[k],
            "tile",
            to,
        )

    def holder(k):
        return behind(k) if k % 2 == 0 else lax.rem(mate + nt - (k - 1), nt)

    def dir_copy(k, part):
        owner = holder(k)
        return remote(
            mine if k == 0 else place(owner, q),
            place(owner, part),
            dir_send.at[k],
            dir_recv.at[k],
            "dir",
            across,
        )

    def core_copy(k, slot, part):
        owner = holder(k)
        source = mine if k == 0 and slot == 0 else place(owner, part)
        return remote(
            source,
            place(owner, part),
            core_send.at[slot, k],
            core_recv.at[slot, k],
            "dir",
            partner,
        )

    def src_copy(k, owner, to):
        return remote(
            src_in.at[span(to * rows, rows)],
            src_all.at[span(owner * pitch, rows)],
            src_send.at[k],
            src_recv.at[k],
            "tile",
            to,
        )

    evens = range(2, nt, 2)
    for k in evens:
        col_copy(k, me, ahead(k)).start()
    row_copy(0, me, mate).start()
    dir_copy(0, q).start()
    core_copy(0, 0, q).start()
    for k in evens:
        src_copy(k, me, ahead(k)).start()
    own = [
        pltpu.make_async_copy(mine, place(me, q), own_sem.at[0]),
        pltpu.make_async_copy(
            src_in.at[span(me * rows, rows)], src_all.at[span(me * pitch, rows)], own_sem.at[1]
        ),
    ]
    for copy in own:
        copy.start()
    for k in evens:
        col_copy(k, behind(k), behind(k)).wait_recv()
        row_copy(k, me, mate).start()
        dir_copy(k, q).start()
        core_copy(k, 0, q).start()
    for k in range(1, nt, 2):
        src_copy(k, me, ahead(k)).start()
    for k in range(0, nt, 2):
        row_copy(k, mate, mate).wait_recv()
        dir_copy(k + 1, q).start()
        core_copy(k + 1, 0, q).start()
    sent = list(range(0, nt, 2)) + list(range(1, nt, 2))
    for k in sent:
        dir_copy(k, across).wait_recv()
        core_copy(k, 1, across).start()
    own[0].wait()
    for k in sent:
        core_copy(k, 0, partner).wait_recv()
        core_copy(k, 1, lax.rem(partner + nd // 2, nd)).wait_recv()

    sub = lax.broadcasted_iota(jnp.int32, (SUBL, LANES), 0)
    lane = lax.broadcasted_iota(jnp.int32, (SUBL, LANES), 1)
    sub_lo, sub_hi = sub > 0, sub < SUBL - 1
    lane_lo, lane_hi = lane > 0, lane < LANES - 1
    zero = jnp.zeros((SUBL, LANES), jnp.float32)

    def down(v):
        return jnp.where(sub_lo, pltpu.roll(v, 1, 0), 0.0)

    def up(v):
        return jnp.where(sub_hi, pltpu.roll(v, SUBL - 1, 0), 0.0)

    def next_z(v):
        return pltpu.roll(v, LANES - 1, 1)

    def prev_z(v):
        return pltpu.roll(v, 1, 1)

    def halo(field):
        for y in range(ny):
            field[0, y] = down(field[nx, y])
            field[nx + 1, y] = up(field[1, y])

    def planes(step, init):
        return lax.fori_loop(0, nx, step, init)

    part_planes = nx // nd

    def table_row(x):
        block = x // part_planes
        return block * piece + (x - block * part_planes) * ny

    def lookup(x, _):
        base = table_row(x)
        for y in range(ny):
            perm_f[x + 1, y] = pm_all[pl.ds(base + y, SUBL, stride=pm_pitch), :]
            mat = pm_all[pl.ds(base + quarter + y, SUBL, stride=pm_pitch), :]
            storage, alpha, bulk, shear = zero, zero, zero, zero
            for c in range(NCLASS):
                hit = mat == float(c)
                storage = jnp.where(hit, tables[0, c], storage)
                alpha = jnp.where(hit, tables[1, c], alpha)
                bulk = jnp.where(hit, tables[2, c], bulk)
                shear = jnp.where(hit, tables[3, c], shear)
            stab = alpha * alpha / bulk
            stab_f[x, y] = stab
            diag_f[x, y] = storage + stab
            hb_f[x, y] = 0.5 * alpha
            shear_f[x + 1, y] = shear
        return 0

    planes(lookup, 0)

    for coef, cs, cx, cy, cz, diag in (
        (perm_f, pcs, pcx, pcy, pcz, diag_f),
        (shear_f, ecs, ecx, ecy, ecz, None),
    ):
        halo(coef)

        def faces(x, _):
            for y in range(ny):
                mid = coef[x + 1, y]
                after = coef[x + 2, y]
                total = coef[x, y] + after
                nz_val = jnp.where(lane_hi, next_z(mid), 0.0)
                total = total + nz_val + jnp.where(lane_lo, prev_z(mid), 0.0)
                if y > 0:
                    total = total + coef[x + 1, y - 1]
                if y < ny - 1:
                    right = coef[x + 1, y + 1]
                    total = total + right
                    cy[x, y] = 0.5 * (mid + right)
                else:
                    cy[x, y] = zero
                cz[x, y] = jnp.where(lane_hi, 0.5 * (mid + nz_val), 0.0)
                face = 0.5 * (mid + after)
                cx[x + 1, y] = jnp.where(jnp.logical_or(x < nx - 1, sub_hi), face, 0.0)
                value = 3.0 * mid + 0.5 * total
                if diag is not None:
                    value = value + diag[x, y]
                cs[x, y] = value
            return 0

        planes(faces, 0)
        for y in range(ny):
            cx[0, y] = down(cx[nx, y])

    def stencil(fields, index, coefs, x, emit, carry):
        cs, cx, cy, cz = coefs
        count = len(index)
        before = [None] * count
        here = [fields(i, x + 1, 0) for i in range(count)]
        cy_before = None
        for y in range(ny):
            s, c_next, c_prev = cs[x, y], cx[x + 1, y], cx[x, y]
            c_y, c_z = cy[x, y], cz[x, y]
            images = []
            centers = []
            for i in range(count):
                v = here[i]
                out = s * v - c_next * fields(i, x + 2, y) - c_prev * fields(i, x, y)
                out = out - (c_z * next_z(v) + prev_z(c_z * v))
                if y > 0:
                    out = out - cy_before * before[i]
                after = None
                if y < ny - 1:
                    after = fields(i, x + 1, y + 1)
                    out = out - c_y * after
                images.append(out)
                centers.append(v)
                before[i], here[i] = v, after
            cy_before = c_y
            carry = emit(y, centers, images, carry)
        return carry

    def single(field):
        return lambda i, x, y: field[x, y]

    def triple(field):
        return lambda i, x, y: field[i, x, y]

    press = (pcs, pcx, pcy, pcz)
    elast = (ecs, ecx, ecy, ecz)

    def first_apply(fields, index, coefs, store):
        def step(x, carry):
            def emit(y, centers, images, acc):
                a, b = acc
                for i in index:
                    store(i, x, y, images[i])
                    a = a + centers[i] * centers[i]
                    b = b + centers[i] * images[i]
                return a, b

            return stencil(fields, index, coefs, x, emit, carry)

        a, b = planes(step, (zero, zero))
        return whole_sum(a), whole_sum(b)

    def second_apply(fields, olds, oldw, index, coefs, beta, store):
        def step(x, carry):
            def emit(y, centers, images, acc):
                for i in index:
                    w = images[i] + beta * oldw(i, x, y)
                    d = centers[i] + beta * olds(i, x + 1, y)
                    acc = acc + d * w
                    if store is not None:
                        store(i, x, y, w)
                return acc

            return stencil(fields, index, coefs, x, emit, carry)

        return whole_sum(planes(step, zero))

    def wb_store(i, x, y, value):
        wb[x, y] = value

    def we_store(i, x, y, value):
        we[i, x, y] = value

    def press_steps(keep):
        halo(r0)
        rr, rw = first_apply(single(r0), (0,), press, wb_store)
        a0 = rr / rw

        def residual(x, acc):
            for y in range(ny):
                v = r0[x + 1, y] - a0 * wb[x, y]
                r1[x + 1, y] = v
                acc = acc + v * v
            return acc

        rr1 = whole_sum(planes(residual, zero))
        beta = rr1 / rr
        halo(r1)
        dw = second_apply(
            single(r1),
            single(r0),
            lambda i, x, y: wb[x, y],
            (0,),
            press,
            beta,
            wb_store if keep else None,
        )
        return a0, rr1 / dw, beta

    for k in range(1, nt):
        src_copy(k, behind(k), behind(k)).wait_recv()
    own[1].wait()

    def take_source(x, _):
        for y in range(ny):
            r0[x + 1, y] = src_all[pl.ds(x * ny + y, SUBL, stride=pitch), :]
        return 0

    planes(take_source, 0)

    def solve(turn, _):
        a0, a1, beta = press_steps(True)
        c0 = a0 + a1 * beta

        def first_press(x, _):
            for y in range(ny):
                old = r1[x + 1, y]
                p = c0 * r0[x + 1, y] + a1 * old
                pb[x + 1, y] = p
                tb[x, y] = old - a1 * wb[x, y] + stab_f[x, y] * p
            return 0

        planes(first_press, 0)
        halo(pb)

        def grad(x, _):
            for y in range(ny):
                b = hb_f[x, y]
                v = pb[x + 1, y]
                eb[0, x + 1, y] = b * (pb[x + 2, y] - pb[x, y])
                hi = pb[x + 1, y + 1] if y < ny - 1 else zero
                lo = pb[x + 1, y - 1] if y > 0 else zero
                eb[1, x + 1, y] = b * (hi - lo)
                eb[2, x + 1, y] = b * (
                    jnp.where(lane_hi, next_z(v), 0.0) - jnp.where(lane_lo, prev_z(v), 0.0)
                )
            return 0

        planes(grad, 0)
        for i in range(3):
            halo(eb.at[i])
        comps = (0, 1, 2)
        rr, rw = first_apply(triple(eb), comps, elast, we_store)
        b0 = rr / rw

        def residual(x, acc):
            for y in range(ny):
                for i in comps:
                    v = eb[i, x + 1, y] - b0 * we[i, x, y]
                    fb[i, x + 1, y] = v
                    acc = acc + v * v
            return acc

        rr1 = whole_sum(planes(residual, zero))
        beta_e = rr1 / rr
        for i in range(3):
            halo(fb.at[i])
        dw = second_apply(
            triple(fb), triple(eb), lambda i, x, y: we[i, x, y], comps, elast, beta_e, None
        )
        b1 = rr1 / dw
        e0 = b0 + b1 * beta_e

        def weigh(x, _):
            for y in range(ny):
                b = hb_f[x, y]
                for i in comps:
                    eb[i, x + 1, y] = b * (e0 * eb[i, x + 1, y] + b1 * fb[i, x + 1, y])
            return 0

        planes(weigh, 0)
        halo(eb.at[0])

        def next_source(x, _):
            for y in range(ny):
                total = tb[x, y] - (eb[0, x, y] - eb[0, x + 2, y])
                if y > 0:
                    total = total - eb[1, x + 1, y - 1]
                if y < ny - 1:
                    total = total + eb[1, x + 1, y + 1]
                w = eb[2, x + 1, y]
                total = total - (
                    jnp.where(lane_lo, prev_z(w), 0.0) - jnp.where(lane_hi, next_z(w), 0.0)
                )
                r0[x + 1, y] = total
            return 0

        planes(next_source, 0)
        a0, a1, beta = press_steps(False)
        c0 = a0 + a1 * beta

        @pl.when(turn == 0)
        def _():
            def last_press(x, _):
                base = table_row(x) + 2 * quarter
                for y in range(ny):
                    p = pb[x + 1, y] + c0 * r0[x + 1, y] + a1 * r1[x + 1, y]
                    r0[x + 1, y] = p * pm_all[pl.ds(base + y, SUBL, stride=pm_pitch), :]
                return 0

            planes(last_press, 0)

        @pl.when(turn == 1)
        def _():
            def last_press(x, _):
                for y in range(ny):
                    p = pb[x + 1, y] + c0 * r0[x + 1, y] + a1 * r1[x + 1, y]
                    out_all[pl.ds(x * ny + y, SUBL, stride=pitch), :] = p
                return 0

            planes(last_press, 0)

        return 0

    lax.fori_loop(0, 2, solve, 0)

    order = [nd // 2] + [m for m in range(1, nd) if m != nd // 2] + [0]

    def ret_copy(m, k, owner, to):
        chunk = lax.rem(q + m, nd)
        return remote(
            out_all.at[span(to * pitch + chunk * quarter, quarter)],
            adj.at[span(owner * rows + chunk * quarter, quarter)],
            ret_send.at[m, k],
            ret_recv.at[m, k],
            "tile",
            to,
        )

    def own_copy(m):
        chunk = lax.rem(q + m, nd)
        return pltpu.make_async_copy(
            out_all.at[span(me * pitch + chunk * quarter, quarter)],
            adj.at[span(me * rows + chunk * quarter, quarter)],
            own_sem.at[m],
        )

    def y_copy(m, k, group, chunk, to):
        owner = behind(k)
        return remote(
            adj.at[span(owner * rows + chunk * quarter, quarter)],
            gat.at[span((group * nt + owner) * gpitch, quarter)],
            y_send.at[m, k],
            y_recv.at[m, k],
            "dir",
            to,
        )

    for m in order:
        own_copy(m).start()
        for k in range(1, nt):
            ret_copy(m, k, me, ahead(k)).start()
    for m in order:
        to = lax.rem(q + m, nd)
        for k in range(nt):
            if k == 0:
                own_copy(m).wait()
            else:
                ret_copy(m, k, behind(k), behind(k)).wait_recv()
            if m > 0:
                y_copy(m, k, q, to, to).start()

    def columns(source, stride, base, group):
        def fill(r, _):
            value = source[pl.ds(base + r, SUBL, stride=stride), :]
            scale = bs_in[pl.ds(q * quarter + r, 1), :]
            ycol[span(group * SUBL, SUBL), pl.ds(pl.multiple_of(r * LANES, LANES), LANES)] = (
                value * scale
            )
            return 0

        lax.fori_loop(0, quarter, fill, 0, unroll=8)

    columns(adj, rows, q * quarter, q)
    for m in order[:-1]:
        group = lax.rem(q + nd - m, nd)
        for k in range(nt):
            y_copy(m, k, group, q, group).wait_recv()
        columns(gat, gpitch, group * nt * gpitch, group)

    nall = nd * nt
    gram = lax.dot_general(
        ycol[...],
        ycol[...],
        (((1,), (1,)), ((), ())),
        precision=lax.Precision.HIGHEST,
        preferred_element_type=jnp.float32,
    )

    def gather_sum(slots, place, send, recv, axis, count):
        def copy(k, owner, to):
            return remote(slots.at[owner], slots.at[owner], send.at[k], recv.at[k], axis, to)

        for k in range(1, count):
            copy(k, place, lax.rem(place + k, count)).start()
        for k in range(1, count):
            owner = lax.rem(place + count - k, count)
            copy(k, owner, owner).wait_recv()
        total = slots[0]
        for s in range(1, count):
            total = total + slots[s]
        for k in range(1, count):
            copy(k, place, lax.rem(place + k, count)).wait_send()
        return total

    part_dir[q] = jnp.zeros((nall, LANES), jnp.float32)
    part_dir[q, :, 0:nall] = gram
    part_tile[me] = gather_sum(part_dir, q, g_send, g_recv, "dir", nd)
    mat = gather_sum(part_tile, me, t_send, t_recv, "tile", nt) / cells

    lanes_all = lax.broadcasted_iota(jnp.int32, (1, LANES), 1)
    for j in range(nall):
        root = jnp.sqrt(mat[j : j + 1, j : j + 1])
        row = mat[j : j + 1, :] / root
        r_out[j : j + 1, :] = jnp.where(lanes_all >= j, row, 0.0)[:, 0:nall]
        mat = mat - (mat[:, j : j + 1] / root) * row

    for k in range(1, nt):
        src_copy(k, me, ahead(k)).wait_send()
        for m in order:
            ret_copy(m, k, me, ahead(k)).wait_send()
    for k in range(nt):
        if k % 2 == 0:
            row_copy(k, me, mate).wait_send()
        if k in evens:
            col_copy(k, me, ahead(k)).wait_send()
        dir_copy(k, q).wait_send()
        core_copy(k, 0, q).wait_send()
        core_copy(k, 1, across).wait_send()
        for m in order[:-1]:
            to = lax.rem(q + m, nd)
            y_copy(m, k, q, to, to).wait_send()


def local_body(
    probes,
    base_sens,
    obs_weight,
    perm,
    material,
    class_storage,
    class_alpha,
    class_bulk,
    class_shear,
):
    nt, nd = lax.axis_size("tile"), lax.axis_size("dir")
    count, nx, ny, nz = probes.shape
    rows = nx * ny
    tables = jnp.stack([class_storage, class_alpha, class_bulk, class_shear])
    source = (base_sens * probes).reshape(count * rows, nz)
    quarter = rows // nd
    coefs = jnp.stack(
        [
            perm.reshape(nd, quarter, nz),
            material.astype(jnp.float32).reshape(nd, quarter, nz),
            obs_weight.reshape(nd, quarter, nz),
        ],
        axis=1,
    ).reshape(3 * rows, nz)
    nall = nd * count
    vmem = pl.BlockSpec(memory_space=pltpu.VMEM)
    f32 = jnp.float32

    def rowbuf(n):
        return pltpu.VMEM((n, nz), f32)

    def field(n):
        return pltpu.VMEM((n, ny, SUBL, LANES), f32)

    def fields(n):
        return pltpu.VMEM((3, n, ny, SUBL, LANES), f32)

    sems = pltpu.SemaphoreType.DMA
    inner_f, outer_f = field(nx), field(nx + 2)
    scratch = [
        rowbuf(nt * (rows + PAD)),
        rowbuf(nt * (3 * rows + PAD)),
        rowbuf(nt * (rows + PAD)),
        rowbuf(nall * (quarter + PAD)),
        pltpu.VMEM((nall, quarter * nz), f32),
        pltpu.VMEM((nd, nall, LANES), f32),
        pltpu.VMEM((nt, nall, LANES), f32),
        outer_f,
        outer_f,
        inner_f,
        inner_f,
        inner_f,
        inner_f,
        field(nx + 1),
        inner_f,
        inner_f,
        inner_f,
        field(nx + 1),
        inner_f,
        inner_f,
        outer_f,
        outer_f,
        outer_f,
        inner_f,
        inner_f,
        fields(nx + 2),
        fields(nx + 2),
        fields(nx),
        sems((nt,)),
        sems((nt,)),
        sems((nt,)),
        sems((nt,)),
        sems((nt,)),
        sems((nt,)),
        sems((2, nt)),
        sems((2, nt)),
        sems((nt,)),
        sems((nt,)),
        sems((nd, nt)),
        sems((nd, nt)),
        sems((nd, nt)),
        sems((nd, nt)),
        sems((nd,)),
        sems((nd,)),
        sems((nt,)),
        sems((nt,)),
        sems((max(nd, 3),)),
    ]
    adjoint, r_factor = pl.pallas_call(
        functools.partial(kernel, (nt, nd, nx, ny, float(nt * rows * nz))),
        out_shape=(
            jax.ShapeDtypeStruct((count * rows, nz), f32),
            jax.ShapeDtypeStruct((nall, nall), f32),
        ),
        in_specs=[pl.BlockSpec(memory_space=pltpu.SMEM)] + [vmem] * 3,
        out_specs=(vmem, vmem),
        scratch_shapes=scratch,
        compiler_params=pltpu.CompilerParams(
            collective_id=0, has_side_effects=True, vmem_limit_bytes=60 * 1024 * 1024
        ),
    )(tables, source, coefs, base_sens.reshape(rows, nz))
    return (base_sens * adjoint.reshape(probes.shape), r_factor)


def body(probes, *others):
    nt, nd = lax.axis_size("tile"), lax.axis_size("dir")
    count, nx, ny, nz = probes.shape
    fits = nt == SUBL and count == nt and nz == LANES and nd == 4 and nx % nd == 0
    fits = fits and ny % 8 == 0 and (nx * ny) % (8 * nd) == 0 and nd * nt <= LANES
    fits = fits and nx * ny * nz <= 32768
    return (local_body if fits else halo_body)(probes, *others)


def solution(mesh):
    placed = (
        P("dir", "tile", None, None),
        P("tile", None, None),
        P("tile", None, None),
        P("tile", None, None),
        P("tile", None, None),
        P(),
        P(),
        P(),
        P(),
    )
    return jax.shard_map(
        body,
        mesh=mesh,
        in_specs=placed,
        out_specs=(P("dir", "tile", None, None), P()),
        check_vma=False,
    )
```

```python
import functools

import jax
import jax.numpy as jnp
from jax import lax
from jax.experimental import pallas as pl
from jax.experimental.pallas import tpu as pltpu
from jax.sharding import PartitionSpec as P

NCLASS = 8
SWEEPS = 2
STEPS = 2


def extended(cells, sides, width):
    for axis, dim in sides:
        count = lax.axis_size(axis)
        ends = count - 1
        head = lax.slice_in_dim(cells, 0, width, axis=dim)
        tail = lax.slice_in_dim(cells, cells.shape[dim] - width, cells.shape[dim], axis=dim)
        cells = jnp.concatenate(
            [
                lax.ppermute(tail, axis, [(i, (i + 1) % count) for i in range(ends)]),
                cells,
                lax.ppermute(head, axis, [((i + 1) % count, i) for i in range(ends)]),
            ],
            axis=dim,
        )
    return cells


def pad_second(field):
    return jnp.pad(field, [(0, 0)] * (field.ndim - 2) + [(1, 1), (0, 0)])


def pad_third(field):
    return jnp.pad(field, [(0, 0)] * (field.ndim - 1) + [(1, 1)])


def face_flux(padded, coef_pad):
    center = padded[..., 1:-1, :, :]
    coef_mid = coef_pad[1:-1]
    result = 0.5 * (coef_mid + coef_pad[2:]) * (center - padded[..., 2:, :, :])
    result = result + 0.5 * (coef_mid + coef_pad[:-2]) * (center - padded[..., :-2, :, :])
    field_y = pad_second(center)
    coef_y = pad_second(coef_mid)
    result = result + 0.5 * (coef_mid + coef_y[:, 2:]) * (center - field_y[..., 2:, :])
    result = result + 0.5 * (coef_mid + coef_y[:, :-2]) * (center - field_y[..., :-2, :])
    field_z = pad_third(center)
    coef_z = pad_third(coef_mid)
    result = result + 0.5 * (coef_mid + coef_z[:, :, 2:]) * (center - field_z[..., 2:])
    result = result + 0.5 * (coef_mid + coef_z[:, :, :-2]) * (center - field_z[..., :-2])
    return result


def gradient(press_pad, biot):
    first = 0.5 * biot * (press_pad[..., 2:, :, :] - press_pad[..., :-2, :, :])
    center = press_pad[..., 1:-1, :, :]
    field_y = pad_second(center)
    second = 0.5 * biot * (field_y[..., 2:, :] - field_y[..., :-2, :])
    field_z = pad_third(center)
    third = 0.5 * biot * (field_z[..., 2:] - field_z[..., :-2])
    return jnp.stack([first, second, third])


def divergence(first_pad, others, biot_pad):
    weighted = biot_pad * first_pad
    result = 0.5 * (weighted[..., :-2, :, :] - weighted[..., 2:, :, :])
    biot = biot_pad[1:-1]
    second = pad_second(biot * others[0])
    result = result + 0.5 * (second[..., :-2, :] - second[..., 2:, :])
    third = pad_third(biot * others[1])
    result = result + 0.5 * (third[..., :-2] - third[..., 2:])
    return result


def inner(left, right):
    summed = jnp.sum(left * right, axis=(-3, -2, -1))
    if summed.ndim == 2:
        summed = jnp.sum(summed, axis=0)
    return lax.psum(summed, "tile")


def spread(values):
    return values[:, None, None, None]


def pad_scalar(field):
    return extended(field, (("tile", 1),), 1)


def pad_vector(field):
    return extended(field, (("tile", 2),), 1)


def conj_grad(operate, extend, target, iterate, iter_pad):
    if iterate is None:
        residual = target
        iterate = jnp.zeros_like(target)
    else:
        residual = target - operate(iter_pad)
    direction = residual
    norm_now = inner(residual, residual)
    for step in range(STEPS):
        image = operate(extend(direction))
        step_len = norm_now / inner(direction, image)
        iterate = iterate + spread(step_len) * direction
        if step + 1 < STEPS:
            residual = residual - spread(step_len) * image
            norm_next = inner(residual, residual)
            direction = residual + spread(norm_next / norm_now) * direction
            norm_now = norm_next
    return iterate


def halo_body(
    probes,
    base_sens,
    obs_weight,
    perm,
    material,
    class_storage,
    class_alpha,
    class_bulk,
    class_shear,
):
    class_mask = (
        material[None] == jnp.arange(NCLASS, dtype=jnp.int32)[:, None, None, None]
    ).astype(jnp.float32)
    storage = jnp.sum(class_storage[:, None, None, None] * class_mask, axis=0)
    biot = jnp.sum(class_alpha[:, None, None, None] * class_mask, axis=0)
    bulk = jnp.sum(class_bulk[:, None, None, None] * class_mask, axis=0)
    shear = jnp.sum(class_shear[:, None, None, None] * class_mask, axis=0)
    stab_term = biot * biot / bulk
    diagonal = storage + stab_term
    coef_all = extended(jnp.stack([perm, biot, shear]), (("tile", 1),), 1)
    perm_pad = coef_all[0]
    biot_pad = coef_all[1]
    shear_pad = coef_all[2]

    def press_apply(padded):
        return diagonal * padded[..., 1:-1, :, :] + face_flux(padded, perm_pad)

    def elast_apply(padded):
        return face_flux(padded, shear_pad)

    def solve(source, orient):
        pressure = None
        displace = None
        press_pad = None
        for sweep in range(SWEEPS):
            source_term = source
            press_init = None
            disp_pad = None
            if displace is not None:
                first_pad = pad_scalar(displace[0])
                press_init = pad_scalar(pressure)
                source_term = (
                    source
                    - orient * divergence(first_pad, (displace[1], displace[2]), biot_pad)
                    + stab_term * pressure
                )
            pressure = conj_grad(press_apply, pad_scalar, source_term, pressure, press_init)
            press_pad = pad_scalar(pressure)
            elastic_term = orient * gradient(press_pad, biot)
            if displace is not None and disp_pad is None:
                disp_pad = pad_vector(displace)
            displace = conj_grad(elast_apply, pad_vector, elastic_term, displace, disp_pad)
        return pressure

    tangent = solve(base_sens * probes, 1.0)
    adjoint = solve(obs_weight * tangent, -1.0)
    hess_block = base_sens * adjoint
    cell_count = (
        hess_block.shape[1] * lax.axis_size("tile") * hess_block.shape[2] * hess_block.shape[3]
    )
    regrouped = lax.all_to_all(hess_block, "dir", split_axis=2, concat_axis=0, tiled=True)
    columns = regrouped.reshape(regrouped.shape[0], -1)
    gram_local = (
        jnp.dot(
            columns, columns.T, precision=lax.Precision.HIGHEST, preferred_element_type=jnp.float32
        )
        / cell_count
    )
    gram_whole = lax.psum(gram_local, ("tile", "dir"))
    r_factor = jnp.linalg.cholesky(gram_whole).T
    return (hess_block, r_factor)

MESH = pl.DeviceIdType.MESH
SUBL = 8
LANES = 128
PAD = 8


def whole_sum(acc):
    return jnp.sum(jnp.sum(acc, axis=1, keepdims=True), axis=0, keepdims=True)


def kernel(
    dims,
    tables,
    probes_in,
    pm_in,
    bs_in,
    adj,
    r_out,
    src_in,
    src_all,
    pm_all,
    out_all,
    gat,
    ycol,
    part_dir,
    part_tile,
    perm_f,
    shear_f,
    diag_f,
    stab_f,
    hb_f,
    pcs,
    pcx,
    pcy,
    pcz,
    ecs,
    ecx,
    ecy,
    ecz,
    r0,
    r1,
    pb,
    wb,
    tb,
    eb,
    fb,
    we,
    col_send,
    col_recv,
    row_send,
    row_recv,
    dir_send,
    dir_recv,
    core_send,
    core_recv,
    src_send,
    src_recv,
    ret_send,
    ret_recv,
    y_send,
    y_recv,
    g_send,
    g_recv,
    t_send,
    t_recv,
    own_sem,
):
    nt, nd, nx, ny, cells = dims
    rows = nx * ny
    quarter = rows // nd
    piece = 3 * quarter
    pitch = rows + PAD
    pm_pitch = 3 * rows + PAD
    gpitch = quarter + PAD
    me = lax.axis_index("tile")
    q = lax.axis_index("dir")
    core = lax.rem(q, 2)
    partner = q + 1 - 2 * core
    across = lax.rem(q + nd // 2, nd)
    mate = me + 1 - 2 * lax.rem(me, 2)

    def span(start, size):
        return pl.ds(pl.multiple_of(start, 8), size)

    def ahead(k):
        return lax.rem(me + k, nt)

    def behind(k):
        return lax.rem(me + nt - k, nt)

    def scale_source(r, _):
        scale = bs_in[span(r * SUBL, SUBL), :]
        for d in range(nt):
            at = span(d * rows + r * SUBL, SUBL)
            src_in[at, :] = probes_in[at, :] * scale
        return 0

    lax.fori_loop(0, rows // SUBL, scale_source, 0)

    barrier = pltpu.get_barrier_semaphore()
    for k in range(1, nt):
        pl.semaphore_signal(barrier, inc=1, device_id={"tile": ahead(k)}, device_id_type=MESH)
    for m in range(1, nd):
        pl.semaphore_signal(
            barrier, inc=1, device_id={"dir": lax.rem(q + m, nd)}, device_id_type=MESH
        )
    pl.semaphore_wait(barrier, nt + nd - 2)

    def remote(src, dst, send, recv, axis, to):
        return pltpu.make_async_remote_copy(
            src_ref=src,
            dst_ref=dst,
            send_sem=send,
            recv_sem=recv,
            device_id={axis: to},
            device_id_type=MESH,
        )

    def place(owner, part):
        return pm_all.at[span(owner * pm_pitch + part * piece, piece)]

    mine = pm_in.at[span(q * piece, piece)]

    def col_copy(k, owner, to):
        return remote(mine, place(owner, q), col_send.at[k], col_recv.at[k], "tile", to)

    def row_copy(k, base, to):
        owner = lax.rem(base + nt - k, nt)
        return remote(
            mine if k == 0 else place(owner, q),
            place(owner, q),
            row_send.at[k],
            row_recv.at[k],
            "tile",
            to,
        )

    def holder(k):
        return behind(k) if k % 2 == 0 else lax.rem(mate + nt - (k - 1), nt)

    def dir_copy(k, part):
        owner = holder(k)
        return remote(
            mine if k == 0 else place(owner, q),
            place(owner, part),
            dir_send.at[k],
            dir_recv.at[k],
            "dir",
            across,
        )

    def core_copy(k, slot, part):
        owner = holder(k)
        source = mine if k == 0 and slot == 0 else place(owner, part)
        return remote(
            source,
            place(owner, part),
            core_send.at[slot, k],
            core_recv.at[slot, k],
            "dir",
            partner,
        )

    def src_copy(k, owner, to):
        return remote(
            src_in.at[span(to * rows, rows)],
            src_all.at[span(owner * pitch, rows)],
            src_send.at[k],
            src_recv.at[k],
            "tile",
            to,
        )

    evens = range(2, nt, 2)
    for k in evens:
        col_copy(k, me, ahead(k)).start()
    row_copy(0, me, mate).start()
    dir_copy(0, q).start()
    core_copy(0, 0, q).start()
    for k in evens:
        src_copy(k, me, ahead(k)).start()
    own = [
        pltpu.make_async_copy(mine, place(me, q), own_sem.at[0]),
        pltpu.make_async_copy(
            src_in.at[span(me * rows, rows)], src_all.at[span(me * pitch, rows)], own_sem.at[1]
        ),
    ]
    for copy in own:
        copy.start()
    for k in evens:
        col_copy(k, behind(k), behind(k)).wait_recv()
        row_copy(k, me, mate).start()
        dir_copy(k, q).start()
        core_copy(k, 0, q).start()
    for k in range(1, nt, 2):
        src_copy(k, me, ahead(k)).start()
    for k in range(0, nt, 2):
        row_copy(k, mate, mate).wait_recv()
        dir_copy(k + 1, q).start()
        core_copy(k + 1, 0, q).start()
    sent = list(range(0, nt, 2)) + list(range(1, nt, 2))
    for k in sent:
        dir_copy(k, across).wait_recv()
        core_copy(k, 1, across).start()
    own[0].wait()
    for k in sent:
        core_copy(k, 0, partner).wait_recv()
        core_copy(k, 1, lax.rem(partner + nd // 2, nd)).wait_recv()

    sub = lax.broadcasted_iota(jnp.int32, (SUBL, LANES), 0)
    lane = lax.broadcasted_iota(jnp.int32, (SUBL, LANES), 1)
    sub_lo, sub_hi = sub > 0, sub < SUBL - 1
    lane_lo, lane_hi = lane > 0, lane < LANES - 1
    zero = jnp.zeros((SUBL, LANES), jnp.float32)

    def down(v):
        return jnp.where(sub_lo, pltpu.roll(v, 1, 0), 0.0)

    def up(v):
        return jnp.where(sub_hi, pltpu.roll(v, SUBL - 1, 0), 0.0)

    def next_z(v):
        return pltpu.roll(v, LANES - 1, 1)

    def prev_z(v):
        return pltpu.roll(v, 1, 1)

    def halo(field):
        for y in range(ny):
            field[0, y] = down(field[nx, y])
            field[nx + 1, y] = up(field[1, y])

    def planes(step, init):
        return lax.fori_loop(0, nx, step, init)

    part_planes = nx // nd

    def table_row(x):
        block = x // part_planes
        return block * piece + (x - block * part_planes) * ny

    def lookup(x, _):
        base = table_row(x)
        for y in range(ny):
            perm_f[x + 1, y] = pm_all[pl.ds(base + y, SUBL, stride=pm_pitch), :]
            mat = pm_all[pl.ds(base + quarter + y, SUBL, stride=pm_pitch), :]
            storage, alpha, bulk, shear = zero, zero, zero, zero
            for c in range(NCLASS):
                hit = mat == float(c)
                storage = jnp.where(hit, tables[0, c], storage)
                alpha = jnp.where(hit, tables[1, c], alpha)
                bulk = jnp.where(hit, tables[2, c], bulk)
                shear = jnp.where(hit, tables[3, c], shear)
            stab = alpha * alpha / bulk
            stab_f[x, y] = stab
            diag_f[x, y] = storage + stab
            hb_f[x, y] = 0.5 * alpha
            shear_f[x + 1, y] = shear
        return 0

    planes(lookup, 0)

    for coef, cs, cx, cy, cz, diag in (
        (perm_f, pcs, pcx, pcy, pcz, diag_f),
        (shear_f, ecs, ecx, ecy, ecz, None),
    ):
        halo(coef)

        def faces(x, _):
            for y in range(ny):
                mid = coef[x + 1, y]
                after = coef[x + 2, y]
                total = coef[x, y] + after
                nz_val = jnp.where(lane_hi, next_z(mid), 0.0)
                total = total + nz_val + jnp.where(lane_lo, prev_z(mid), 0.0)
                if y > 0:
                    total = total + coef[x + 1, y - 1]
                if y < ny - 1:
                    right = coef[x + 1, y + 1]
                    total = total + right
                    cy[x, y] = 0.5 * (mid + right)
                else:
                    cy[x, y] = zero
                cz[x, y] = jnp.where(lane_hi, 0.5 * (mid + nz_val), 0.0)
                face = 0.5 * (mid + after)
                cx[x + 1, y] = jnp.where(jnp.logical_or(x < nx - 1, sub_hi), face, 0.0)
                value = 3.0 * mid + 0.5 * total
                if diag is not None:
                    value = value + diag[x, y]
                cs[x, y] = value
            return 0

        planes(faces, 0)
        for y in range(ny):
            cx[0, y] = down(cx[nx, y])

    def stencil(fields, index, coefs, x, emit, carry):
        cs, cx, cy, cz = coefs
        count = len(index)
        before = [None] * count
        here = [fields(i, x + 1, 0) for i in range(count)]
        cy_before = None
        for y in range(ny):
            s, c_next, c_prev = cs[x, y], cx[x + 1, y], cx[x, y]
            c_y, c_z = cy[x, y], cz[x, y]
            images = []
            centers = []
            for i in range(count):
                v = here[i]
                out = s * v - c_next * fields(i, x + 2, y) - c_prev * fields(i, x, y)
                out = out - (c_z * next_z(v) + prev_z(c_z * v))
                if y > 0:
                    out = out - cy_before * before[i]
                after = None
                if y < ny - 1:
                    after = fields(i, x + 1, y + 1)
                    out = out - c_y * after
                images.append(out)
                centers.append(v)
                before[i], here[i] = v, after
            cy_before = c_y
            carry = emit(y, centers, images, carry)
        return carry

    def single(field):
        return lambda i, x, y: field[x, y]

    def triple(field):
        return lambda i, x, y: field[i, x, y]

    press = (pcs, pcx, pcy, pcz)
    elast = (ecs, ecx, ecy, ecz)

    def first_apply(fields, index, coefs, store):
        def step(x, carry):
            def emit(y, centers, images, acc):
                a, b = acc
                for i in index:
                    store(i, x, y, images[i])
                    a = a + centers[i] * centers[i]
                    b = b + centers[i] * images[i]
                return a, b

            return stencil(fields, index, coefs, x, emit, carry)

        a, b = planes(step, (zero, zero))
        return whole_sum(a), whole_sum(b)

    def second_apply(fields, olds, oldw, index, coefs, beta, store):
        def step(x, carry):
            def emit(y, centers, images, acc):
                for i in index:
                    w = images[i] + beta * oldw(i, x, y)
                    d = centers[i] + beta * olds(i, x + 1, y)
                    acc = acc + d * w
                    if store is not None:
                        store(i, x, y, w)
                return acc

            return stencil(fields, index, coefs, x, emit, carry)

        return whole_sum(planes(step, zero))

    def wb_store(i, x, y, value):
        wb[x, y] = value

    def we_store(i, x, y, value):
        we[i, x, y] = value

    def press_steps(keep):
        halo(r0)
        rr, rw = first_apply(single(r0), (0,), press, wb_store)
        a0 = rr / rw

        def residual(x, acc):
            for y in range(ny):
                v = r0[x + 1, y] - a0 * wb[x, y]
                r1[x + 1, y] = v
                acc = acc + v * v
            return acc

        rr1 = whole_sum(planes(residual, zero))
        beta = rr1 / rr
        halo(r1)
        dw = second_apply(
            single(r1),
            single(r0),
            lambda i, x, y: wb[x, y],
            (0,),
            press,
            beta,
            wb_store if keep else None,
        )
        return a0, rr1 / dw, beta

    for k in range(1, nt):
        src_copy(k, behind(k), behind(k)).wait_recv()
    own[1].wait()

    def take_source(x, _):
        for y in range(ny):
            r0[x + 1, y] = src_all[pl.ds(x * ny + y, SUBL, stride=pitch), :]
        return 0

    planes(take_source, 0)

    def solve(turn, _):
        a0, a1, beta = press_steps(True)
        c0 = a0 + a1 * beta

        def first_press(x, _):
            for y in range(ny):
                old = r1[x + 1, y]
                p = c0 * r0[x + 1, y] + a1 * old
                pb[x + 1, y] = p
                tb[x, y] = old - a1 * wb[x, y] + stab_f[x, y] * p
            return 0

        planes(first_press, 0)
        halo(pb)

        def grad(x, _):
            for y in range(ny):
                b = hb_f[x, y]
                v = pb[x + 1, y]
                eb[0, x + 1, y] = b * (pb[x + 2, y] - pb[x, y])
                hi = pb[x + 1, y + 1] if y < ny - 1 else zero
                lo = pb[x + 1, y - 1] if y > 0 else zero
                eb[1, x + 1, y] = b * (hi - lo)
                eb[2, x + 1, y] = b * (
                    jnp.where(lane_hi, next_z(v), 0.0) - jnp.where(lane_lo, prev_z(v), 0.0)
                )
            return 0

        planes(grad, 0)
        for i in range(3):
            halo(eb.at[i])
        comps = (0, 1, 2)
        rr, rw = first_apply(triple(eb), comps, elast, we_store)
        b0 = rr / rw

        def residual(x, acc):
            for y in range(ny):
                for i in comps:
                    v = eb[i, x + 1, y] - b0 * we[i, x, y]
                    fb[i, x + 1, y] = v
                    acc = acc + v * v
            return acc

        rr1 = whole_sum(planes(residual, zero))
        beta_e = rr1 / rr
        for i in range(3):
            halo(fb.at[i])
        dw = second_apply(
            triple(fb), triple(eb), lambda i, x, y: we[i, x, y], comps, elast, beta_e, None
        )
        b1 = rr1 / dw
        e0 = b0 + b1 * beta_e

        def weigh(x, _):
            for y in range(ny):
                b = hb_f[x, y]
                for i in comps:
                    eb[i, x + 1, y] = b * (e0 * eb[i, x + 1, y] + b1 * fb[i, x + 1, y])
            return 0

        planes(weigh, 0)
        halo(eb.at[0])

        def next_source(x, _):
            for y in range(ny):
                total = tb[x, y] - (eb[0, x, y] - eb[0, x + 2, y])
                if y > 0:
                    total = total - eb[1, x + 1, y - 1]
                if y < ny - 1:
                    total = total + eb[1, x + 1, y + 1]
                w = eb[2, x + 1, y]
                total = total - (
                    jnp.where(lane_lo, prev_z(w), 0.0) - jnp.where(lane_hi, next_z(w), 0.0)
                )
                r0[x + 1, y] = total
            return 0

        planes(next_source, 0)
        a0, a1, beta = press_steps(False)
        c0 = a0 + a1 * beta

        @pl.when(turn == 0)
        def _():
            def last_press(x, _):
                base = table_row(x) + 2 * quarter
                for y in range(ny):
                    p = pb[x + 1, y] + c0 * r0[x + 1, y] + a1 * r1[x + 1, y]
                    r0[x + 1, y] = p * pm_all[pl.ds(base + y, SUBL, stride=pm_pitch), :]
                return 0

            planes(last_press, 0)

        @pl.when(turn == 1)
        def _():
            def last_press(x, _):
                for y in range(ny):
                    p = pb[x + 1, y] + c0 * r0[x + 1, y] + a1 * r1[x + 1, y]
                    out_all[pl.ds(x * ny + y, SUBL, stride=pitch), :] = p
                return 0

            planes(last_press, 0)

        return 0

    lax.fori_loop(0, 2, solve, 0)

    order = [nd // 2] + [m for m in range(1, nd) if m != nd // 2] + [0]

    def ret_copy(m, k, owner, to):
        chunk = lax.rem(q + m, nd)
        return remote(
            out_all.at[span(to * pitch + chunk * quarter, quarter)],
            adj.at[span(owner * rows + chunk * quarter, quarter)],
            ret_send.at[m, k],
            ret_recv.at[m, k],
            "tile",
            to,
        )

    def own_copy(m):
        chunk = lax.rem(q + m, nd)
        return pltpu.make_async_copy(
            out_all.at[span(me * pitch + chunk * quarter, quarter)],
            adj.at[span(me * rows + chunk * quarter, quarter)],
            own_sem.at[m],
        )

    def y_copy(m, k, group, chunk, to):
        owner = behind(k)
        return remote(
            adj.at[span(owner * rows + chunk * quarter, quarter)],
            gat.at[span((group * nt + owner) * gpitch, quarter)],
            y_send.at[m, k],
            y_recv.at[m, k],
            "dir",
            to,
        )

    for m in order:
        own_copy(m).start()
        for k in range(1, nt):
            ret_copy(m, k, me, ahead(k)).start()
    for m in order:
        to = lax.rem(q + m, nd)
        for k in range(nt):
            if k == 0:
                own_copy(m).wait()
            else:
                ret_copy(m, k, behind(k), behind(k)).wait_recv()
            if m > 0:
                y_copy(m, k, q, to, to).start()

    def columns(source, stride, base, group):
        def fill(r, _):
            value = source[pl.ds(base + r, SUBL, stride=stride), :]
            scale = bs_in[pl.ds(q * quarter + r, 1), :]
            ycol[span(group * SUBL, SUBL), pl.ds(pl.multiple_of(r * LANES, LANES), LANES)] = (
                value * scale
            )
            return 0

        lax.fori_loop(0, quarter, fill, 0, unroll=8)

    columns(adj, rows, q * quarter, q)
    for m in order[:-1]:
        group = lax.rem(q + nd - m, nd)
        for k in range(nt):
            y_copy(m, k, group, q, group).wait_recv()
        columns(gat, gpitch, group * nt * gpitch, group)

    nall = nd * nt
    gram = lax.dot_general(
        ycol[...],
        ycol[...],
        (((1,), (1,)), ((), ())),
        precision=lax.Precision.HIGHEST,
        preferred_element_type=jnp.float32,
    )

    def gather_sum(slots, place, send, recv, axis, count):
        def copy(k, owner, to):
            return remote(slots.at[owner], slots.at[owner], send.at[k], recv.at[k], axis, to)

        for k in range(1, count):
            copy(k, place, lax.rem(place + k, count)).start()
        for k in range(1, count):
            owner = lax.rem(place + count - k, count)
            copy(k, owner, owner).wait_recv()
        total = slots[0]
        for s in range(1, count):
            total = total + slots[s]
        for k in range(1, count):
            copy(k, place, lax.rem(place + k, count)).wait_send()
        return total

    part_dir[q] = jnp.zeros((nall, LANES), jnp.float32)
    part_dir[q, :, 0:nall] = gram
    part_tile[me] = gather_sum(part_dir, q, g_send, g_recv, "dir", nd)
    mat = gather_sum(part_tile, me, t_send, t_recv, "tile", nt) / cells

    lanes_all = lax.broadcasted_iota(jnp.int32, (1, LANES), 1)
    for j in range(nall):
        root = jnp.sqrt(mat[j : j + 1, j : j + 1])
        row = mat[j : j + 1, :] / root
        r_out[j : j + 1, :] = jnp.where(lanes_all >= j, row, 0.0)[:, 0:nall]
        mat = mat - (mat[:, j : j + 1] / root) * row

    for k in range(1, nt):
        src_copy(k, me, ahead(k)).wait_send()
        for m in order:
            ret_copy(m, k, me, ahead(k)).wait_send()
    for k in range(nt):
        if k % 2 == 0:
            row_copy(k, me, mate).wait_send()
        if k in evens:
            col_copy(k, me, ahead(k)).wait_send()
        dir_copy(k, q).wait_send()
        core_copy(k, 0, q).wait_send()
        core_copy(k, 1, across).wait_send()
        for m in order[:-1]:
            to = lax.rem(q + m, nd)
            y_copy(m, k, q, to, to).wait_send()


def local_body(
    probes,
    base_sens,
    obs_weight,
    perm,
    material,
    class_storage,
    class_alpha,
    class_bulk,
    class_shear,
):
    nt, nd = lax.axis_size("tile"), lax.axis_size("dir")
    count, nx, ny, nz = probes.shape
    rows = nx * ny
    tables = jnp.stack([class_storage, class_alpha, class_bulk, class_shear])
    source = probes.reshape(count * rows, nz)
    quarter = rows // nd
    coefs = jnp.stack(
        [
            perm.reshape(nd, quarter, nz),
            material.astype(jnp.float32).reshape(nd, quarter, nz),
            obs_weight.reshape(nd, quarter, nz),
        ],
        axis=1,
    ).reshape(3 * rows, nz)
    nall = nd * count
    vmem = pl.BlockSpec(memory_space=pltpu.VMEM)
    f32 = jnp.float32

    def rowbuf(n):
        return pltpu.VMEM((n, nz), f32)

    def field(n):
        return pltpu.VMEM((n, ny, SUBL, LANES), f32)

    def fields(n):
        return pltpu.VMEM((3, n, ny, SUBL, LANES), f32)

    sems = pltpu.SemaphoreType.DMA
    inner_f, outer_f = field(nx), field(nx + 2)
    scratch = [
        rowbuf(count * rows),
        rowbuf(nt * (rows + PAD)),
        rowbuf(nt * (3 * rows + PAD)),
        rowbuf(nt * (rows + PAD)),
        rowbuf(nall * (quarter + PAD)),
        pltpu.VMEM((nall, quarter * nz), f32),
        pltpu.VMEM((nd, nall, LANES), f32),
        pltpu.VMEM((nt, nall, LANES), f32),
        outer_f,
        outer_f,
        inner_f,
        inner_f,
        inner_f,
        inner_f,
        field(nx + 1),
        inner_f,
        inner_f,
        inner_f,
        field(nx + 1),
        inner_f,
        inner_f,
        outer_f,
        outer_f,
        outer_f,
        inner_f,
        inner_f,
        fields(nx + 2),
        fields(nx + 2),
        fields(nx),
        sems((nt,)),
        sems((nt,)),
        sems((nt,)),
        sems((nt,)),
        sems((nt,)),
        sems((nt,)),
        sems((2, nt)),
        sems((2, nt)),
        sems((nt,)),
        sems((nt,)),
        sems((nd, nt)),
        sems((nd, nt)),
        sems((nd, nt)),
        sems((nd, nt)),
        sems((nd,)),
        sems((nd,)),
        sems((nt,)),
        sems((nt,)),
        sems((max(nd, 3),)),
    ]
    adjoint, r_factor = pl.pallas_call(
        functools.partial(kernel, (nt, nd, nx, ny, float(nt * rows * nz))),
        out_shape=(
            jax.ShapeDtypeStruct((count * rows, nz), f32),
            jax.ShapeDtypeStruct((nall, nall), f32),
        ),
        in_specs=[pl.BlockSpec(memory_space=pltpu.SMEM)] + [vmem] * 3,
        out_specs=(vmem, vmem),
        scratch_shapes=scratch,
        compiler_params=pltpu.CompilerParams(
            collective_id=0, has_side_effects=True, vmem_limit_bytes=60 * 1024 * 1024
        ),
    )(tables, source, coefs, base_sens.reshape(rows, nz))
    return (base_sens * adjoint.reshape(probes.shape), r_factor)


def body(probes, *others):
    nt, nd = lax.axis_size("tile"), lax.axis_size("dir")
    count, nx, ny, nz = probes.shape
    fits = nt == SUBL and count == nt and nz == LANES and nd == 4 and nx % nd == 0
    fits = fits and ny % 8 == 0 and (nx * ny) % (8 * nd) == 0 and nd * nt <= LANES
    fits = fits and nx * ny * nz <= 32768
    return (local_body if fits else halo_body)(probes, *others)


def solution(mesh):
    placed = (
        P("dir", "tile", None, None),
        P("tile", None, None),
        P("tile", None, None),
        P("tile", None, None),
        P("tile", None, None),
        P(),
        P(),
        P(),
        P(),
    )
    return jax.shard_map(
        body,
        mesh=mesh,
        in_specs=placed,
        out_specs=(P("dir", "tile", None, None), P()),
        check_vma=False,
    )
```
